256 devices in a mesh: groups: 4 (over y, x), expert: 64 (over z, core).
Axes of the slice: x: 2, y: 2, z: 32, core: 2. Of those that a mesh axis runs over, the one named last changes fastest.
The devices are a block of a 4x8x32 slice.
Arguments:
- tokens: bfloat16 [32768, 4096], P(('groups', 'expert')), parts along dimension 0, may hold values from -6 to 6
- router_weight: bfloat16 [4096, 128], replicated, may hold values from -0.078125 to 0.078125
- expert_ids: int32 [32768, 8], P(('groups', 'expert')), parts along dimension 0, may hold values from 0 to 127, all different within a row; in each aligned block of 128 rows (0 to 127, 128 to 255, ...) at most 9 rows name the same one
Outputs:
- expert_rows: bfloat16 [128, 2304, 4096], P('expert', 'groups'), parts along dimension 1
- balance_loss: float32 [4], P('groups'), parts along dimension 0
The draws below stay inside these ranges and needn't reach their ends.
There are 4 independent parts, one for each index of `groups`. The reference program is written for one: setup_inputs(seed, part) draws one part's arguments, and reference() takes and returns one part's arrays. A program takes and returns all parts, laid end to end along the dimension named above; an argument that names none is the same for every part. Nothing has to cross between parts.
Inputs may be any that keep to these rules, and one draw needn't show every extreme that they name: `expert_ids`: each row names 8 different experts; among the rows of one device no expert is named more than 9 times, a bound that some block reaches.
All inputs are finite; a program needn't handle non-finite values.
Results may differ from the reference program's by a relative error of at most 0.0012.
Values may be sent and summed in bfloat16 or wider, within the bound.
No kernel may reach another device: no remote copies, remote signals or barrier semaphores. Data moves between devices by JAX's collectives and lax.ppermute only.
A program may use at most 128 MiB of HBM per device.

```python
import math
import jax
import jax.numpy as jnp
import numpy as np

D = 4096
EXPERTS = 128
TOP_K = 8
TOK_DEV = 128
CAP = 9
TOKENS = 8192
SLOTS = 576
N_EXPERT = 64


def pattern_signs(count):
    index = jnp.arange(count, dtype=jnp.int32)
    parity = jnp.zeros((count,), jnp.int32)
    for bit_place in range(20):
        parity = parity + jnp.bitwise_and(jnp.right_shift(index, bit_place), 1)
    return 1.0 - 2.0 * jnp.bitwise_and(parity, 1).astype(jnp.float32)


def draw_router_weight(key, part):
    first = jax.random.fold_in(key, 11)
    second = jax.random.fold_in(key, 12)
    noise = jnp.clip(jax.random.normal(first, (D, EXPERTS), jnp.float32), -4.0, 4.0)
    amplitude = jax.random.uniform(second, (EXPERTS,), jnp.float32, 0.3, 1.0)
    combined = (noise + amplitude[None, :] * pattern_signs(D)[:, None]) * D ** (-0.5)
    return combined.astype(jnp.bfloat16)


def draw_tokens(key, part):
    first = jax.random.fold_in(key, 21)
    second = jax.random.fold_in(key, 22)
    third = jax.random.fold_in(key, 23)
    rise = jnp.arange(TOKENS, dtype=jnp.float32) / max(TOKENS - 1, 1)
    base = jnp.clip(jax.random.normal(first, (TOKENS, D), jnp.float32), -6.0, 6.0)
    share = 1.0 / 32.0 * jnp.exp(rise * jnp.log(8.0))
    chosen_rows = jax.random.uniform(second, (TOKENS,), jnp.float32) < share
    strength = jax.random.randint(third, (TOKENS,), 2, 7).astype(jnp.float32)
    planted = strength[:, None] * pattern_signs(D)[None, :]
    return jnp.where(chosen_rows[:, None], planted, base).astype(jnp.bfloat16)


def deal_out(rng, own, number, rows, number_of, top, reach, lean):
    order = jax.random.permutation(rng, number_of)
    crowded, usual = load_shares(number_of, rows * top, reach, lean, True), load_shares(number_of, rows * top, reach, lean, False)
    places = jnp.arange(number_of)

    def named(tallies, offset_by):
        used = int((tallies > 0).sum())
        fixed = max(1, used // 4)
        moved = fixed + (places - fixed + offset_by * (used - fixed)) % max(1, number_of - fixed)
        return jnp.zeros((number_of,), jnp.int32).at[order[jnp.where(places < fixed, places, moved)]].set(jnp.asarray(tallies, jnp.int32))

    tallies = jnp.where(number % 4 == 0, named(crowded, number // 4), named(usual, number - number // 4 - 1))
    mixed = jax.random.permutation(jax.random.fold_in(own, 3), number_of)
    giver, receiver = mixed[0:number_of // 2 * 2:2], mixed[1:number_of // 2 * 2:2]
    slack = jnp.minimum(tallies[giver] - 1, reach - tallies[receiver]) // 2
    slack = jnp.where((giver == order[0]) | (receiver == order[0]) | (tallies[receiver] == 0), 0, jnp.maximum(slack, 0))
    moved = jax.random.randint(jax.random.fold_in(own, 4), (number_of // 2,), 0, 1 << 20) % (slack + 1)
    tallies = tallies.at[giver].add(-moved).at[receiver].add(moved)
    members = jnp.searchsorted(jnp.cumsum(tallies), jnp.arange(rows * top), side="right").astype(jnp.int32)
    listing = members.reshape(top, rows).T
    listing = listing[jax.random.permutation(jax.random.fold_in(own, 1), rows)]
    offset_by = jax.random.randint(jax.random.fold_in(own, 2), (rows, 1), 0, top)
    return jnp.take_along_axis(listing, (jnp.arange(top)[None, :] + offset_by) % top, axis=1)


def load_shares(count, total, bound, skew, full):
    weights = [(1 << 20) // math.isqrt(standing ** skew) + 1 for standing in range(1, count + 1)]
    largest = bound if full else min(bound, max(-(-total // count), total * weights[0] // sum(weights)))
    least = 1 if total - largest >= count - 1 else 0
    counts, surplus = [largest] + [least] * (count - 1), total - largest - least * (count - 1)
    while surplus > 0:
        candidates = [i for i in range(1, count) if counts[i] < largest] or [i for i in range(1, count) if counts[i] < bound]
        mass, left = sum([weights[i] for i in candidates]), surplus
        for i in candidates:
            more = min(bound - counts[i], max(1, left * weights[i] // mass), surplus)
            counts[i] = counts[i] + more
            surplus = surplus - more
    return np.array(counts)


def setup_inputs(seed: int = 0, part: int = 0) -> dict:
    keys = jax.random.split(jax.random.key(seed), 4)
    part_splits = jax.random.split(jax.random.fold_in(keys[3], part), 4)
    tokens = draw_tokens(jax.random.fold_in(jax.random.fold_in(keys[3], part), 71), part)
    router_weight = draw_router_weight(jax.random.fold_in(keys[3], 71), part)
    expert_ids_keys = jax.random.split(jax.random.fold_in(part_splits[2], 1), TOKENS // TOK_DEV)
    expert_ids_turns = jax.random.permutation(jax.random.fold_in(part_splits[2], 3), TOKENS // TOK_DEV)
    expert_ids = jax.vmap(lambda own, number: deal_out(jax.random.fold_in(part_splits[2], 2), own, number, TOK_DEV, EXPERTS, TOP_K, CAP, 2))(expert_ids_keys, expert_ids_turns).reshape((TOKENS, TOP_K))
    return dict(tokens=tokens, router_weight=router_weight, expert_ids=expert_ids)


def reference(tokens, router_weight, expert_ids):
    logits = jnp.dot(tokens, router_weight, preferred_element_type=jnp.float32)
    probability = jax.nn.softmax(logits, axis=-1)
    chosen = jnp.take_along_axis(logits, expert_ids, axis=1)
    gates = jax.nn.softmax(chosen, axis=1)
    onehot = jnp.sum((expert_ids[:, :, None] == jnp.arange(EXPERTS, dtype=jnp.int32)[None, None, :]).astype(jnp.int32), axis=1).astype(jnp.int32)
    blocks = onehot.reshape(N_EXPERT, TOK_DEV, EXPERTS)
    before = (jnp.cumsum(blocks, axis=1) - blocks).astype(jnp.int32).reshape(TOKENS, EXPERTS)
    slot_rank = jnp.take_along_axis(before, expert_ids, axis=1).astype(jnp.int32)
    owner_index = (jnp.arange(TOKENS, dtype=jnp.int32) // TOK_DEV)[:, None]
    position = (owner_index * CAP + slot_rank).astype(jnp.int32)
    widened = tokens.astype(jnp.float32)
    expert_rows = jnp.zeros((EXPERTS, SLOTS, D), jnp.bfloat16)
    for column in range(TOP_K):
        gated = (gates[:, column:column + 1] * widened).astype(jnp.bfloat16)
        expert_rows = expert_rows.at[expert_ids[:, column], position[:, column]].set(gated)
    expert_load = jnp.sum(onehot, axis=0).astype(jnp.float32)
    expert_mass = jnp.sum(probability, axis=0)
    token_total = jnp.float32(TOKENS)
    balance_loss = EXPERTS * jnp.sum(expert_load * expert_mass) / (token_total * token_total * TOP_K)
    return expert_rows, balance_loss.reshape(1)
```

```python
import functools

import jax
import jax.numpy as jnp
from jax import lax
from jax.experimental import pallas as pl
from jax.experimental.pallas import tpu as pltpu
from jax.sharding import Mesh
from jax.sharding import PartitionSpec as P

EXPERTS = 128
TOP_K = 8
CAP = 9
WIN = 24
EXPERT = ("chip", "core")
ALL = ("groups", "chip", "core")


def far_keys(away, reach, back):
    return [
        jnp.where((d >= 1) & (d <= r), d, 0).astype(jnp.float32)
        for d, r in ((away, reach), (away, reach - 1), (back, reach - 1), (back, reach))
    ]


def keys_of(ids, z, chips, per_chip, axis):
    away = lax.rem(ids // per_chip - z + chips, chips)
    back = lax.rem(chips - away, chips)
    return [
        jnp.max(k, axis=axis, keepdims=True) for k in far_keys(away, chips // 2, back)
    ]


def order_body(chips, per_chip, z_ref, ids_ref, idst_ref, tok_ref, *outs):
    rows, width = tok_ref.shape
    half = width // 2
    z = z_ref[0]
    cols = keys_of(ids_ref[...], z, chips, per_chip, 1)
    lanes = keys_of(idst_ref[...], z, chips, per_chip, 0)
    u = lax.broadcasted_iota(jnp.int32, (rows, rows), 0)
    t = lax.broadcasted_iota(jnp.int32, (rows, rows), 1)
    for which, (kc, kr) in enumerate(zip(cols, lanes)):
        ahead = (kc > kr) | ((kc == kr) & (u < t))
        place = jnp.sum(ahead.astype(jnp.float32), axis=0, keepdims=True)
        pick = (u.astype(jnp.float32) == place).astype(jnp.bfloat16)
        at = (which % 2) * half
        outs[which][...] = jnp.dot(
            pick, tok_ref[:, at : at + half], preferred_element_type=jnp.float32
        ).astype(jnp.bfloat16)


def route_body(chips, per_chip, z_ref, ids_ref, idst_ref, tok_ref, w_ref, tab_ref):
    rows = tok_ref.shape[0]
    reach = chips // 2
    z = z_ref[0]
    ids = ids_ref[...]
    logits = jnp.dot(tok_ref[...], w_ref[...], preferred_element_type=jnp.float32)
    e = lax.broadcasted_iota(jnp.int32, (rows, EXPERTS), 1)
    named = ids[:, 0:1] == e
    for k in range(1, TOP_K):
        named = named | (ids[:, k : k + 1] == e)
    top = jnp.max(logits, axis=1, keepdims=True)
    ex = jnp.exp(logits - top)
    probability = ex / jnp.sum(ex, axis=1, keepdims=True)
    best = jnp.max(jnp.where(named, logits, -jnp.inf), axis=1, keepdims=True)
    ge = jnp.exp(jnp.where(named, logits - best, -jnp.inf))
    gates = ge / jnp.sum(ge, axis=1, keepdims=True)
    count = named.astype(jnp.float32)
    u = lax.broadcasted_iota(jnp.int32, (rows, rows), 0)
    t = lax.broadcasted_iota(jnp.int32, (rows, rows), 1)
    lower = (t < u).astype(jnp.bfloat16)
    before = jnp.dot(lower, count.astype(jnp.bfloat16), preferred_element_type=jnp.float32)
    cols = keys_of(ids, z, chips, per_chip, 1)
    lanes = keys_of(idst_ref[...], z, chips, per_chip, 0)
    places = []
    for kc, kr in zip(cols, lanes):
        ahead = (kr > kc) | ((kr == kc) & (t < u))
        places.append(jnp.sum(ahead.astype(jnp.float32), axis=1, keepdims=True))
    away = lax.rem(e // per_chip - z + chips, chips)
    lo = jnp.where(away <= reach, places[0], places[2]) + 1.0
    hi = jnp.where(away < reach, places[1], places[3]) + 1.0
    for r in range(CAP):
        here = named & (before == r)
        for at, value, shift in ((0, lo, 1.0), (1, hi, 1.0), (2, gates, 0.0)):
            row = jnp.sum(jnp.where(here, value, 0.0), axis=0, keepdims=True) - shift
            tab_ref[at * CAP + r : at * CAP + r + 1, :] = row
    tab_ref[3 * CAP : 3 * CAP + 1, :] = jnp.sum(count, axis=0, keepdims=True)
    tab_ref[3 * CAP + 1 : 3 * CAP + 2, :] = jnp.sum(probability, axis=0, keepdims=True)
    tab_ref[3 * CAP + 2 :, :] = jnp.zeros((tab_ref.shape[0] - 3 * CAP - 2, EXPERTS), jnp.float32)


def place_body(plan, per_dev, sc_ref, *refs):
    n_src = len(plan)
    tabs = refs[:n_src]
    n_arr = 1 + max(i for src in plan for piece in src for i in piece)
    arrs = refs[n_src : n_src + n_arr]
    out_ref = refs[n_src + n_arr + 1]
    buf, sem = refs[n_src + n_arr + 2 :]
    core = sc_ref[n_src]
    wide = out_ref.shape[2]
    half = wide // 2
    step = 512

    def window(s, e):
        first = pl.multiple_of(((CAP * sc_ref[s]) // 4) * 8, 8)
        return out_ref.at[e, pl.ds(first, WIN), :]

    for s in range(n_src):
        for e in range(per_dev):
            k = s * per_dev + e
            pltpu.make_async_copy(window(s, e), buf.at[k], sem.at[k]).start()
    for s in range(n_src):
        for e in range(per_dev):
            k = s * per_dev + e
            pltpu.make_async_copy(window(s, e), buf.at[k], sem.at[k]).wait()
    for s in range(n_src):
        shift = lax.rem(2 * CAP * sc_ref[s], 8)
        w = lax.broadcasted_iota(jnp.int32, (WIN, step), 0) - shift
        mine = (w >= 0) & (w < 2 * CAP)
        for piece in range(2):
            own, peer = plan[s][piece]
            own_ref, peer_ref = arrs[own], arrs[peer]
            n = own_ref.shape[0]
            spot = tabs[s][0, :, piece : piece + 1]
            gate = tabs[s][0, :, 2:3]
            row = lax.broadcasted_iota(jnp.int32, (per_dev * WIN, n), 1).astype(jnp.float32)
            mine_f = (core * 128).astype(jnp.float32)
            peer_f = ((1 - core) * 128).astype(jnp.float32)
            s_own = (row == spot - mine_f).astype(jnp.bfloat16)
            s_peer = (row == spot - peer_f).astype(jnp.bfloat16)

            def column(i, carry, s=s, piece=piece, own_ref=own_ref, peer_ref=peer_ref,
                       s_own=s_own, s_peer=s_peer, gate=gate, mine=mine):
                c = pl.multiple_of(i * step, step)
                acc = jnp.dot(s_own, own_ref[:, pl.ds(c, step)], preferred_element_type=jnp.float32)
                acc = acc + jnp.dot(s_peer, peer_ref[:, pl.ds(c, step)], preferred_element_type=jnp.float32)
                acc = acc * gate
                at = pl.multiple_of(piece * half + i * step, step)
                for e in range(per_dev):
                    k = s * per_dev + e
                    old = buf[k, :, pl.ds(at, step)].astype(jnp.float32)
                    new = jnp.where(mine, acc[e * WIN : (e + 1) * WIN, :], old)
                    buf[k, :, pl.ds(at, step)] = new.astype(jnp.bfloat16)
                return carry

            lax.fori_loop(0, half // step, column, 0)
    for s in range(n_src):
        for e in range(per_dev):
            k = s * per_dev + e
            pltpu.make_async_copy(buf.at[k], window(s, e), sem.at[k]).start()
    for s in range(n_src):
        for e in range(per_dev):
            k = s * per_dev + e
            pltpu.make_async_copy(buf.at[k], window(s, e), sem.at[k]).wait()


def place(out, table, sources, core, plan, arrays):
    per_dev = out.shape[0]
    n_src = len(plan)
    scalars = jnp.stack([*sources, core]).astype(jnp.int32)

    def tab_spec(s):
        return pl.BlockSpec((1, *table.shape[1:]), lambda i, sc: (sc[s], 0, 0))

    whole = [pl.BlockSpec(a.shape, lambda i, sc: (0, 0)) for a in arrays]
    return pl.pallas_call(
        functools.partial(place_body, plan, per_dev),
        grid_spec=pltpu.PrefetchScalarGridSpec(
            num_scalar_prefetch=1,
            grid=(1,),
            in_specs=[*(tab_spec(s) for s in range(n_src)), *whole, pl.BlockSpec(memory_space=pl.ANY)],
            out_specs=pl.BlockSpec(memory_space=pl.ANY),
            scratch_shapes=[
                pltpu.VMEM((n_src * per_dev, WIN, out.shape[2]), out.dtype),
                pltpu.SemaphoreType.DMA((n_src * per_dev,)),
            ],
        ),
        out_shape=jax.ShapeDtypeStruct(out.shape, out.dtype),
        input_output_aliases={1 + n_src + len(arrays): 0},
        name="place",
    )(scalars, *([table] * n_src), *arrays, out)


def whole_call(body, scalar, arrays, shapes):
    spec = lambda a: pl.BlockSpec(a.shape, lambda: (0,) * len(a.shape))
    return pl.pallas_call(
        body,
        in_specs=[pl.BlockSpec(memory_space=pltpu.SMEM), *(spec(a) for a in arrays)],
        out_specs=[spec(s) for s in shapes],
        out_shape=shapes,
    )(scalar, *arrays)


def trade(message, totals, chips):
    core = lax.axis_index("core")
    z = lax.axis_index("chip")
    lanes = message.shape[-1]
    bits = chips.bit_length() - 1
    steps = [("core", 0, core)] + [("chip", k, z) for k in range(bits)]
    data = message.reshape(2 * chips, 1, lanes)
    blocks = 2 * chips
    seen = 1
    for axis, bit, index in steps:
        mine = (index >> bit) & 1
        data = data.reshape(blocks // 2, 2, seen, lanes)
        keep = lax.dynamic_index_in_dim(data, mine, 1, keepdims=False)
        give = lax.dynamic_index_in_dim(data, 1 - mine, 1, keepdims=False)
        rows = (blocks // 2) * seen
        packed = jnp.concatenate([give.reshape(rows, lanes), totals], axis=0)
        size = lax.axis_size(axis)
        got = lax.ppermute(packed, axis, [(i, i ^ (1 << bit)) for i in range(size)])
        totals = totals + got[rows:]
        came = got[:rows].reshape(blocks // 2, seen, lanes)
        low = jnp.where(mine == 0, keep, came)
        high = jnp.where(mine == 0, came, keep)
        data = jnp.stack([low, high], axis=1).reshape(blocks // 2, 2 * seen, lanes)
        blocks //= 2
        seen *= 2
    return data.reshape(seen, lanes), totals


def layer(tokens, router_weight, expert_ids):
    chips = lax.axis_size("chip")
    reach = chips // 2
    local_rows, width = tokens.shape
    half = width // 2
    per_dev = EXPERTS // (2 * chips)
    per_chip = 2 * per_dev
    slots_chip = per_chip * CAP
    z = lax.axis_index("chip")
    core = lax.axis_index("core")
    onward = [(i, (i + 1) % chips) for i in range(chips)]
    backward = [(i, (i - 1) % chips) for i in range(chips)]

    def send(x, to):
        return lax.ppermute(x, "chip", to)

    def swap(x):
        return lax.ppermute(x, "core", [(0, 1), (1, 0)])

    def need(h, far):
        rows = slots_chip * (far - h + 1)
        return min(local_rows, (rows + 7) // 8 * 8)

    ids_t = expert_ids.T
    zs = z.astype(jnp.int32).reshape(1)
    sds = jax.ShapeDtypeStruct
    flows = whole_call(
        functools.partial(order_body, chips, per_chip), zs,
        (expert_ids, ids_t, tokens), [sds((local_rows, half), tokens.dtype)] * 4,
    )
    (table,) = whole_call(
        functools.partial(route_body, chips, per_chip), zs,
        (expert_ids, ids_t, tokens, router_weight), [sds((32, EXPERTS), jnp.float32)],
    )
    rows = 3 * CAP
    message = table[:rows].reshape(rows, 2 * chips, per_dev).transpose(1, 2, 0)
    message = message.reshape(2 * chips, per_dev * rows)
    message = jnp.pad(message, ((0, 0), (0, 128 - per_dev * rows)))
    got, totals = trade(message, table[rows : rows + 2], chips)
    token_total = jnp.float32(local_rows * 2 * chips)
    loss = EXPERTS * jnp.sum(totals[0] * totals[1]) / (token_total * token_total * TOP_K)

    got = got[:, : per_dev * rows].reshape(chips, 2, per_dev, 3, CAP)
    bump = jnp.arange(2, dtype=jnp.float32)[None, :, None, None, None] * local_rows
    is_spot = (jnp.arange(3) < 2)[None, None, None, :, None]
    got = jnp.where(is_spot & (got >= 0), got + bump, got)
    got = got.transpose(0, 2, 1, 4, 3).reshape(chips // 4, 4, per_dev, 2 * CAP, 3)
    blank = jnp.array([-1.0, -1.0, 0.0], jnp.float32)
    moved = []
    for q in range(4):
        lead = (2 * CAP * q) % 8
        shape = lambda n: (chips // 4, per_dev, n, 3)
        moved.append(
            jnp.concatenate(
                [
                    jnp.broadcast_to(blank, shape(lead)),
                    got[:, q],
                    jnp.broadcast_to(blank, shape(WIN - lead - 2 * CAP)),
                ],
                axis=2,
            )
        )
    windows = jnp.stack(moved, axis=1).reshape(chips, per_dev * WIN, 3)
    windows = jnp.pad(windows, ((0, 0), (0, 0), (0, 5)))

    out = jnp.zeros((per_dev, 2 * chips * CAP, width), tokens.dtype)
    own = (flows[0], swap(flows[0]), flows[1], swap(flows[1]))
    out = place(out, windows, [z], core, (((0, 1), (2, 3)),), own)
    fars = (reach, reach - 1, reach - 1, reach)
    ways = (onward, onward, backward, backward)
    for h in range(1, reach + 1):
        up, down = (z - h) % chips, (z + h) % chips
        sent = []
        for x, far, way in zip(flows, fars, ways):
            if h <= far:
                x = send(x[: need(h, far)], way)
                sent.append(x)
            else:
                sent.append(None)
        flows = sent
        live = [x for x in flows if x is not None]
        arrays = tuple(y for x in live for y in (x, swap(x)))
        if h < reach:
            plan = (((0, 1), (2, 3)), ((4, 5), (6, 7)))
            out = place(out, windows, [up, down], core, plan, arrays)
        else:
            out = place(out, windows, [up], core, (((0, 1), (2, 3)),), arrays)
    return out, loss.reshape(1)


def solution(mesh):
    finer = Mesh(mesh.devices.reshape(mesh.shape["groups"], -1, 2), ALL)
    in_specs = (P(ALL, None), P(), P(ALL, None))
    out_specs = (P(EXPERT, "groups", None), P("groups"))
    return jax.shard_map(layer, mesh=finer, in_specs=in_specs, out_specs=out_specs, check_vma=False)
```

```python
import functools

import jax
import jax.numpy as jnp
from jax import lax
from jax.experimental import pallas as pl
from jax.experimental.pallas import tpu as pltpu
from jax.sharding import Mesh
from jax.sharding import PartitionSpec as P

EXPERTS = 128
TOP_K = 8
CAP = 9
WIN = 24
EXPERT = ("chip", "core")
ALL = ("groups", "chip", "core")


def far_keys(away, reach, back):
    return [
        jnp.where((d >= 1) & (d <= r), d, 0).astype(jnp.float32)
        for d, r in ((away, reach), (away, reach - 1), (back, reach - 1), (back, reach))
    ]


def keys_of(ids, z, chips, per_chip, axis):
    away = lax.rem(ids // per_chip - z + chips, chips)
    back = lax.rem(chips - away, chips)
    return [
        jnp.max(k, axis=axis, keepdims=True) for k in far_keys(away, chips // 2, back)
    ]


def order_body(chips, per_chip, z_ref, ids_ref, idst_ref, tok_ref, *outs):
    rows, width = tok_ref.shape
    half = width // 2
    z = z_ref[0]
    cols = keys_of(ids_ref[...], z, chips, per_chip, 1)
    lanes = keys_of(idst_ref[...], z, chips, per_chip, 0)
    u = lax.broadcasted_iota(jnp.int32, (rows, rows), 0)
    t = lax.broadcasted_iota(jnp.int32, (rows, rows), 1)
    for which, (kc, kr) in enumerate(zip(cols, lanes)):
        ahead = (kc > kr) | ((kc == kr) & (u < t))
        place = jnp.sum(ahead.astype(jnp.float32), axis=0, keepdims=True)
        pick = (u.astype(jnp.float32) == place).astype(jnp.bfloat16)
        at = (which % 2) * half
        outs[which][...] = jnp.dot(
            pick, tok_ref[:, at : at + half], preferred_element_type=jnp.float32
        ).astype(jnp.bfloat16)


def route_body(chips, per_chip, z_ref, ids_ref, idst_ref, tok_ref, w_ref, tab_ref):
    rows = tok_ref.shape[0]
    reach = chips // 2
    z = z_ref[0]
    ids = ids_ref[...]
    logits = jnp.dot(tok_ref[...], w_ref[...], preferred_element_type=jnp.float32)
    e = lax.broadcasted_iota(jnp.int32, (rows, EXPERTS), 1)
    named = ids[:, 0:1] == e
    for k in range(1, TOP_K):
        named = named | (ids[:, k : k + 1] == e)
    top = jnp.max(logits, axis=1, keepdims=True)
    ex = jnp.exp(logits - top)
    probability = ex / jnp.sum(ex, axis=1, keepdims=True)
    best = jnp.max(jnp.where(named, logits, -jnp.inf), axis=1, keepdims=True)
    ge = jnp.exp(jnp.where(named, logits - best, -jnp.inf))
    gates = ge / jnp.sum(ge, axis=1, keepdims=True)
    count = named.astype(jnp.float32)
    u = lax.broadcasted_iota(jnp.int32, (rows, rows), 0)
    t = lax.broadcasted_iota(jnp.int32, (rows, rows), 1)
    lower = (t < u).astype(jnp.bfloat16)
    before = jnp.dot(lower, count.astype(jnp.bfloat16), preferred_element_type=jnp.float32)
    cols = keys_of(ids, z, chips, per_chip, 1)
    lanes = keys_of(idst_ref[...], z, chips, per_chip, 0)
    places = []
    for kc, kr in zip(cols, lanes):
        ahead = (kr > kc) | ((kr == kc) & (t < u))
        places.append(jnp.sum(ahead.astype(jnp.float32), axis=1, keepdims=True))
    away = lax.rem(e // per_chip - z + chips, chips)
    lo = jnp.where(away <= reach, places[0], places[2]) + 1.0
    hi = jnp.where(away < reach, places[1], places[3]) + 1.0
    for r in range(CAP):
        here = named & (before == r)
        for at, value, shift in ((0, lo, 1.0), (1, hi, 1.0), (2, gates, 0.0)):
            row = jnp.sum(jnp.where(here, value, 0.0), axis=0, keepdims=True) - shift
            tab_ref[at * CAP + r : at * CAP + r + 1, :] = row
    tab_ref[3 * CAP : 3 * CAP + 1, :] = jnp.sum(count, axis=0, keepdims=True)
    tab_ref[3 * CAP + 1 : 3 * CAP + 2, :] = jnp.sum(probability, axis=0, keepdims=True)
    tab_ref[3 * CAP + 2 :, :] = jnp.zeros((tab_ref.shape[0] - 3 * CAP - 2, EXPERTS), jnp.float32)


def place_body(n_src, n_old, fresh, per_dev, sc_ref, *refs):
    refs = list(refs)
    take = lambda n: [refs.pop(0) for _ in range(n)]
    tabs, flows = take(n_src), take(2 * n_src)
    keep_old, got_old = take(2) if n_old else (None, None)
    if n_old and not fresh:
        take(1)
    (out_ref,) = take(1) if n_old else (None,)
    keep_ref, give_ref = take(2) if n_src else (None, None)
    step = 512
    span = per_dev * WIN
    if n_old:
        buf, in_sem, out_sem = refs
        wide = out_ref.shape[2]
        spots = [(s, e) for s in range(n_old) for e in range(per_dev)]

        def window(s, e):
            first = pl.multiple_of(((CAP * sc_ref[n_src + s]) // 4) * 8, 8)
            return out_ref.at[e, pl.ds(first, WIN), :]

        def fetch(sources):
            for k, (s, e) in enumerate(spots):
                if s in sources:
                    pltpu.make_async_copy(window(s, e), buf.at[k], in_sem.at[k]).start()

        def settle(sources):
            for k, (s, e) in enumerate(spots):
                if s in sources:
                    pltpu.make_async_copy(buf.at[k], window(s, e), out_sem.at[k]).wait()

        fetch((0, 1))
        for k, (s, e) in enumerate(spots):
            if s == 2 and e == 0:
                settle((0, 1))
                fetch((2,))
            pltpu.make_async_copy(window(s, e), buf.at[k], in_sem.at[k]).wait()
            shift = lax.rem(2 * CAP * sc_ref[n_src + s], 8)
            w = lax.broadcasted_iota(jnp.int32, (WIN, step), 0) - shift
            mine = (w >= 0) & (w < 2 * CAP)

            def merge(i, carry, k=k, mine=mine):
                c = pl.multiple_of(i * step, step)
                here = (pl.ds(k * WIN, WIN), pl.ds(c, step))
                new = keep_old[here].astype(jnp.float32) + got_old[here].astype(jnp.float32)
                old = buf[k, :, pl.ds(c, step)].astype(jnp.float32)
                buf[k, :, pl.ds(c, step)] = jnp.where(mine, new, old).astype(buf.dtype)
                return carry

            lax.fori_loop(0, wide // step, merge, 0)
            pltpu.make_async_copy(buf.at[k], window(s, e), out_sem.at[k]).start()
    for s in range(n_src):
        for piece in range(2):
            flow = flows[2 * s + piece]
            n, half = flow.shape
            spot = tabs[s][0, :, piece : piece + 1]
            gate = tabs[s][0, :, 2:3]
            row = lax.broadcasted_iota(jnp.int32, (2 * span, n), 1).astype(jnp.float32)
            pick = (row == spot).astype(jnp.bfloat16)

            def column(i, carry, s=s, piece=piece, flow=flow, pick=pick, gate=gate, half=half):
                c = pl.multiple_of(i * step, step)
                acc = jnp.dot(pick, flow[:, pl.ds(c, step)], preferred_element_type=jnp.float32)
                acc = (acc * gate).astype(jnp.bfloat16)
                at = pl.multiple_of(piece * half + i * step, step)
                keep_ref[s * span : (s + 1) * span, pl.ds(at, step)] = acc[:span]
                give_ref[s * span : (s + 1) * span, pl.ds(at, step)] = acc[span:]
                return carry

            lax.fori_loop(0, half // step, column, 0)
    if n_old:
        settle((2,) if n_old > 2 else (0, 1))


def place(out, table, sources, flows, old, shape, per_dev):
    n_src = len(sources)
    n_old = len(old[0]) if old else 0
    fresh = out is None
    span = per_dev * WIN
    width = shape.shape[2]
    scalars = jnp.stack([*sources, *(old[0] if old else ())]).astype(jnp.int32)
    flat = lambda a: pl.BlockSpec(a.shape, lambda i, sc: (0, 0))
    anywhere = pl.BlockSpec(memory_space=pl.ANY)
    args, specs, outs, out_specs, scratch, alias = [], [], [], [], [], {}
    for s in range(n_src):
        args.append(table)
        specs.append(pl.BlockSpec((1, *table.shape[1:]), lambda i, sc, s=s: (sc[s], 0, 0)))
    for a in (*flows, *(old[1:] if old else ())):
        args.append(a)
        specs.append(flat(a))
    if n_old:
        if not fresh:
            alias = {1 + len(args): 0}
            args.append(out)
            specs.append(anywhere)
        outs.append(shape)
        out_specs.append(anywhere)
        count = n_old * per_dev
        scratch = [
            pltpu.VMEM((count, WIN, width), shape.dtype),
            pltpu.SemaphoreType.DMA((count,)),
            pltpu.SemaphoreType.DMA((count,)),
        ]
    if n_src:
        block = jax.ShapeDtypeStruct((n_src * span, width), shape.dtype)
        outs += [block, block]
        out_specs += [flat(block), flat(block)]
    result = pl.pallas_call(
        functools.partial(place_body, n_src, n_old, fresh, per_dev),
        grid_spec=pltpu.PrefetchScalarGridSpec(
            num_scalar_prefetch=1, grid=(1,), in_specs=specs, out_specs=out_specs,
            scratch_shapes=scratch,
        ),
        out_shape=outs,
        input_output_aliases=alias,
        name="place",
    )(scalars, *args)
    result = list(result)
    if n_old:
        out = result.pop(0)
    return out, result


def whole_call(body, scalar, arrays, shapes):
    spec = lambda a: pl.BlockSpec(a.shape, lambda: (0,) * len(a.shape))
    return pl.pallas_call(
        body,
        in_specs=[pl.BlockSpec(memory_space=pltpu.SMEM), *(spec(a) for a in arrays)],
        out_specs=[spec(s) for s in shapes],
        out_shape=shapes,
    )(scalar, *arrays)


def trade(message, totals, chips):
    z = lax.axis_index("chip")
    lanes = message.shape[-1]
    data = message
    blocks, seen = chips, 1
    for step in range(chips.bit_length() - 1):
        mine = (z >> step) & 1
        data = data.reshape(blocks // 2, 2, seen, lanes)
        keep = lax.dynamic_index_in_dim(data, mine, 1, keepdims=False)
        give = lax.dynamic_index_in_dim(data, 1 - mine, 1, keepdims=False)
        rows = chips // 2
        packed = jnp.concatenate([give.reshape(rows, lanes), totals], axis=0)
        got = lax.ppermute(packed, "chip", [(i, i ^ (1 << step)) for i in range(chips)])
        totals = totals + got[rows:]
        came = got[:rows].reshape(blocks // 2, seen, lanes)
        low = jnp.where(mine == 0, keep, came)
        high = jnp.where(mine == 0, came, keep)
        data = jnp.stack([low, high], axis=1)
        blocks //= 2
        seen *= 2
    totals = totals + lax.ppermute(totals, "core", [(0, 1), (1, 0)])
    return data.reshape(chips, lanes), totals


def layer(tokens, router_weight, expert_ids):
    chips = lax.axis_size("chip")
    reach = chips // 2
    local_rows, width = tokens.shape
    half = width // 2
    per_dev = EXPERTS // (2 * chips)
    per_chip = 2 * per_dev
    slots_chip = per_chip * CAP
    z = lax.axis_index("chip")
    core = lax.axis_index("core")
    onward = [(i, (i + 1) % chips) for i in range(chips)]
    backward = [(i, (i - 1) % chips) for i in range(chips)]

    def send(x, to):
        return lax.ppermute(x, "chip", to)

    def swap(x):
        return lax.ppermute(x, "core", [(0, 1), (1, 0)])

    def need(h, far):
        if h <= reach - 3:
            return local_rows
        rows = slots_chip * (far - h + 1)
        return min(local_rows, (rows + 7) // 8 * 8)

    ids_t = expert_ids.T
    zs = z.astype(jnp.int32).reshape(1)
    sds = jax.ShapeDtypeStruct
    flows = whole_call(
        functools.partial(order_body, chips, per_chip), zs,
        (expert_ids, ids_t, tokens), [sds((local_rows, half), tokens.dtype)] * 4,
    )
    (table,) = whole_call(
        functools.partial(route_body, chips, per_chip), zs,
        (expert_ids, ids_t, tokens, router_weight), [sds((32, EXPERTS), jnp.float32)],
    )
    rows = 3 * CAP
    message = table[:rows].reshape(rows, chips, per_chip).transpose(1, 2, 0)
    message = message.reshape(chips, per_chip * rows)
    message = jnp.pad(message, ((0, 0), (0, 128 - per_chip * rows)))
    got, totals = trade(message, table[rows : rows + 2], chips)
    token_total = jnp.float32(local_rows * 2 * chips)
    loss = EXPERTS * jnp.sum(totals[0] * totals[1]) / (token_total * token_total * TOP_K)

    blank = jnp.array([-1.0, -1.0, 0.0], jnp.float32)
    got = got[:, : per_chip * rows].reshape(chips, 2, per_dev, 3, CAP)
    got = jnp.where(core == 0, got, got[:, ::-1]).reshape(chips, per_chip, 3, CAP)
    got = got.transpose(0, 1, 3, 2)
    void = jnp.broadcast_to(blank, got.shape)
    got = jnp.concatenate(
        [jnp.where(core == 0, got, void), jnp.where(core == 0, void, got)], axis=2
    ).reshape(chips // 4, 4, per_chip, 2 * CAP, 3)
    moved = []
    for q in range(4):
        lead = (2 * CAP * q) % 8
        shape = lambda n: (chips // 4, per_chip, n, 3)
        moved.append(
            jnp.concatenate(
                [
                    jnp.broadcast_to(blank, shape(lead)),
                    got[:, q],
                    jnp.broadcast_to(blank, shape(WIN - lead - 2 * CAP)),
                ],
                axis=2,
            )
        )
    windows = jnp.stack(moved, axis=1).reshape(chips, per_chip * WIN, 3)
    windows = jnp.pad(windows, ((0, 0), (0, 0), (0, 5)))

    shape = sds((per_dev, 2 * chips * CAP, width), tokens.dtype)
    out, (keep, give) = place(None, windows, [z], flows[:2], None, shape, per_dev)
    old = ([z], keep, swap(give))
    fars = (reach, reach - 1, reach - 1, reach)
    ways = (onward, onward, backward, backward)
    live, sources = [], []
    for h in range(1, reach + 1):
        up, down = (z - h) % chips, (z + h) % chips
        sent = []
        for x, far, way in zip(flows, fars, ways):
            if h <= far:
                x = send(x[: need(h, far)], way)
                sent.append(x)
            else:
                sent.append(None)
        flows = sent
        live += [x for x in flows if x is not None]
        sources += [up, down] if h < reach else [up]
        if h == reach - 1:
            continue
        out, (keep, give) = place(out, windows, sources, live, old, shape, per_dev)
        old = (sources, keep, swap(give))
        live, sources = [], []
    out, _ = place(out, windows, [], [], old, shape, per_dev)
    return out, loss.reshape(1)


def solution(mesh):
    finer = Mesh(mesh.devices.reshape(mesh.shape["groups"], -1, 2), ALL)
    in_specs = (P(ALL, None), P(), P(ALL, None))
    out_specs = (P(EXPERT, "groups", None), P("groups"))
    return jax.shard_map(layer, mesh=finer, in_specs=in_specs, out_specs=out_specs, check_vma=False)
```

```python
import functools

import jax
import jax.numpy as jnp
from jax import lax
from jax.experimental import pallas as pl
from jax.experimental.pallas import tpu as pltpu
from jax.sharding import Mesh
from jax.sharding import PartitionSpec as P

EXPERTS = 128
TOP_K = 8
CAP = 9
WIN = 24
EXPERT = ("chip", "core")
ALL = ("groups", "chip", "core")


def far_keys(away, reach, back):
    return [
        jnp.where((d >= 1) & (d <= r), d, 0).astype(jnp.float32)
        for d, r in ((away, reach), (away, reach - 1), (back, reach - 1), (back, reach))
    ]


def keys_of(ids, z, chips, per_chip, axis):
    away = lax.rem(ids // per_chip - z + chips, chips)
    back = lax.rem(chips - away, chips)
    return [
        jnp.max(k, axis=axis, keepdims=True) for k in far_keys(away, chips // 2, back)
    ]


def order_body(chips, per_chip, z_ref, ids_ref, idst_ref, tok_ref, *outs):
    rows, width = tok_ref.shape
    half = width // 2
    z = z_ref[0]
    cols = keys_of(ids_ref[...], z, chips, per_chip, 1)
    lanes = keys_of(idst_ref[...], z, chips, per_chip, 0)
    u = lax.broadcasted_iota(jnp.int32, (rows, rows), 0)
    t = lax.broadcasted_iota(jnp.int32, (rows, rows), 1)
    for which, (kc, kr) in enumerate(zip(cols, lanes)):
        ahead = (kc > kr) | ((kc == kr) & (u < t))
        place = jnp.sum(ahead.astype(jnp.float32), axis=0, keepdims=True)
        pick = (u.astype(jnp.float32) == place).astype(jnp.bfloat16)
        at = (which % 2) * half
        outs[which][...] = jnp.dot(
            pick, tok_ref[:, at : at + half], preferred_element_type=jnp.float32
        ).astype(jnp.bfloat16)


def route_body(chips, per_chip, z_ref, ids_ref, idst_ref, tok_ref, w_ref, tab_ref):
    rows = tok_ref.shape[0]
    reach = chips // 2
    z = z_ref[0]
    ids = ids_ref[...]
    logits = jnp.dot(tok_ref[...], w_ref[...], preferred_element_type=jnp.float32)
    e = lax.broadcasted_iota(jnp.int32, (rows, EXPERTS), 1)
    named = ids[:, 0:1] == e
    for k in range(1, TOP_K):
        named = named | (ids[:, k : k + 1] == e)
    top = jnp.max(logits, axis=1, keepdims=True)
    ex = jnp.exp(logits - top)
    probability = ex / jnp.sum(ex, axis=1, keepdims=True)
    best = jnp.max(jnp.where(named, logits, -jnp.inf), axis=1, keepdims=True)
    ge = jnp.exp(jnp.where(named, logits - best, -jnp.inf))
    gates = ge / jnp.sum(ge, axis=1, keepdims=True)
    count = named.astype(jnp.float32)
    u = lax.broadcasted_iota(jnp.int32, (rows, rows), 0)
    t = lax.broadcasted_iota(jnp.int32, (rows, rows), 1)
    lower = (t < u).astype(jnp.bfloat16)
    before = jnp.dot(lower, count.astype(jnp.bfloat16), preferred_element_type=jnp.float32)
    cols = keys_of(ids, z, chips, per_chip, 1)
    lanes = keys_of(idst_ref[...], z, chips, per_chip, 0)
    places = []
    for kc, kr in zip(cols, lanes):
        ahead = (kr > kc) | ((kr == kc) & (t < u))
        places.append(jnp.sum(ahead.astype(jnp.float32), axis=1, keepdims=True))
    away = lax.rem(e // per_chip - z + chips, chips)
    lo = jnp.where(away <= reach, places[0], places[2]) + 1.0
    hi = jnp.where(away < reach, places[1], places[3]) + 1.0
    for r in range(CAP):
        here = named & (before == r)
        for at, value, shift in ((0, lo, 1.0), (1, hi, 1.0), (2, gates, 0.0)):
            row = jnp.sum(jnp.where(here, value, 0.0), axis=0, keepdims=True) - shift
            tab_ref[at * CAP + r : at * CAP + r + 1, :] = row
    tab_ref[3 * CAP : 3 * CAP + 1, :] = jnp.sum(count, axis=0, keepdims=True)
    tab_ref[3 * CAP + 1 : 3 * CAP + 2, :] = jnp.sum(probability, axis=0, keepdims=True)
    tab_ref[3 * CAP + 2 :, :] = jnp.zeros((tab_ref.shape[0] - 3 * CAP - 2, EXPERTS), jnp.float32)


def place_body(n_src, n_old, fresh, per_dev, sc_ref, *refs):
    refs = list(refs)
    take = lambda n: [refs.pop(0) for _ in range(n)]
    tabs, flows = take(n_src), take(2 * n_src)
    keep_old, got_old = take(2) if n_old else (None, None)
    if n_old and not fresh:
        take(1)
    (out_ref,) = take(1) if n_old else (None,)
    picked = take(2) if n_src else ()
    span = per_dev * WIN
    if n_old:
        buf, was, in_sem, out_sem, was_sem = take(5)
        wide = out_ref.shape[2]
        spots = [(s, e) for s in range(n_old) for e in range(per_dev)]

        def window(s, e):
            first = pl.multiple_of(((CAP * sc_ref[n_src + s]) // 4) * 8, 8)
            return out_ref.at[e, pl.ds(first, WIN), :]

        def fetch(sources):
            return [
                pltpu.make_async_copy(window(s, e), buf.at[k], in_sem.at[k])
                for k, (s, e) in enumerate(spots)
                if s in sources
            ]

        def store(sources):
            return [
                pltpu.make_async_copy(buf.at[k], window(s, e), out_sem.at[k])
                for k, (s, e) in enumerate(spots)
                if s in sources
            ]

        def earlier(s):
            rows = pl.ds(s * span, span)
            return [
                pltpu.make_async_copy(old.at[rows, :], was.at[i, rows, :], was_sem.at[2 * s + i])
                for i, old in enumerate((keep_old, got_old))
            ]

    if n_src:
        arrived = take(2 * n_src)
        block, flow_sem, block_sem = take(3)
        loads = [
            pltpu.make_async_copy(flow, here, flow_sem.at[k])
            for k, (flow, here) in enumerate(zip(flows, arrived))
        ]
        for load in loads:
            load.start()
    if n_old:
        for copy in fetch((0, 1)):
            copy.start()
        for s in range(n_old):
            for copy in earlier(s):
                copy.start()
    sent = []
    for s in range(n_src):
        for piece in range(2):
            k = 2 * s + piece
            loads[k].wait()
            n, half = arrived[k].shape
            spot = tabs[s][0, :, piece : piece + 1]
            gate = tabs[s][0, :, 2:3]
            row = lax.broadcasted_iota(jnp.int32, (2 * span, n), 1).astype(jnp.float32)
            pick = (row == spot).astype(jnp.bfloat16)
            acc = jnp.dot(pick, arrived[k][...], preferred_element_type=jnp.float32)
            acc = (acc * gate).astype(jnp.bfloat16)
            at = piece * half
            for i in range(2):
                block[i, s * span : (s + 1) * span, at : at + half] = acc[i * span : (i + 1) * span]
        rows = pl.ds(s * span, span)
        for i in range(2):
            copy = pltpu.make_async_copy(
                block.at[i, rows, :], picked[i].at[rows, :], block_sem.at[2 * s + i]
            )
            copy.start()
            sent.append(copy)
    if n_old:
        step = wide // 2
        for k, (s, e) in enumerate(spots):
            if e == 0:
                if s == 2:
                    for copy in store((0, 1)):
                        copy.wait()
                    for copy in fetch((2,)):
                        copy.start()
                for copy in earlier(s):
                    copy.wait()
            pltpu.make_async_copy(window(s, e), buf.at[k], in_sem.at[k]).wait()
            shift = lax.rem(2 * CAP * sc_ref[n_src + s], 8)
            w = lax.broadcasted_iota(jnp.int32, (WIN, step), 0) - shift
            mine = (w >= 0) & (w < 2 * CAP)

            def merge(i, carry, k=k, mine=mine):
                c = pl.multiple_of(i * step, step)
                here = (pl.ds(k * WIN, WIN), pl.ds(c, step))
                new = was[0, here[0], here[1]].astype(jnp.float32)
                new = new + was[1, here[0], here[1]].astype(jnp.float32)
                old = buf[k, :, pl.ds(c, step)].astype(jnp.float32)
                buf[k, :, pl.ds(c, step)] = jnp.where(mine, new, old).astype(buf.dtype)
                return carry

            lax.fori_loop(0, wide // step, merge, 0)
            pltpu.make_async_copy(buf.at[k], window(s, e), out_sem.at[k]).start()
        for copy in store((2,) if n_old > 2 else (0, 1)):
            copy.wait()
    for copy in sent:
        copy.wait()


def place(out, table, sources, flows, old, shape, per_dev):
    n_src = len(sources)
    n_old = len(old[0]) if old else 0
    fresh = out is None
    span = per_dev * WIN
    width = shape.shape[2]
    scalars = jnp.stack([*sources, *(old[0] if old else ())]).astype(jnp.int32)
    anywhere = pl.BlockSpec(memory_space=pl.ANY)
    args, specs, outs, out_specs, scratch, alias = [], [], [], [], [], {}
    for s in range(n_src):
        args.append(table)
        specs.append(pl.BlockSpec((1, *table.shape[1:]), lambda i, sc, s=s: (sc[s], 0, 0)))
    for a in (*flows, *(old[1:] if old else ())):
        args.append(a)
        specs.append(anywhere)
    if n_old:
        if not fresh:
            alias = {1 + len(args): 0}
            args.append(out)
            specs.append(anywhere)
        outs.append(shape)
        out_specs.append(anywhere)
        count = n_old * per_dev
        scratch = [
            pltpu.VMEM((count, WIN, width), shape.dtype),
            pltpu.VMEM((2, n_old * span, width), shape.dtype),
            pltpu.SemaphoreType.DMA((count,)),
            pltpu.SemaphoreType.DMA((count,)),
            pltpu.SemaphoreType.DMA((2 * n_old,)),
        ]
    if n_src:
        block = jax.ShapeDtypeStruct((n_src * span, width), shape.dtype)
        outs += [block, block]
        out_specs += [anywhere, anywhere]
        scratch += [
            *(pltpu.VMEM(a.shape, a.dtype) for a in flows),
            pltpu.VMEM((2, n_src * span, width), shape.dtype),
            pltpu.SemaphoreType.DMA((2 * n_src,)),
            pltpu.SemaphoreType.DMA((2 * n_src,)),
        ]
    result = pl.pallas_call(
        functools.partial(place_body, n_src, n_old, fresh, per_dev),
        grid_spec=pltpu.PrefetchScalarGridSpec(
            num_scalar_prefetch=1, grid=(1,), in_specs=specs, out_specs=out_specs,
            scratch_shapes=scratch,
        ),
        out_shape=outs,
        input_output_aliases=alias,
        name="place",
    )(scalars, *args)
    result = list(result)
    if n_old:
        out = result.pop(0)
    return out, result


def whole_call(body, scalar, arrays, shapes):
    spec = lambda a: pl.BlockSpec(a.shape, lambda: (0,) * len(a.shape))
    return pl.pallas_call(
        body,
        in_specs=[pl.BlockSpec(memory_space=pltpu.SMEM), *(spec(a) for a in arrays)],
        out_specs=[spec(s) for s in shapes],
        out_shape=shapes,
    )(scalar, *arrays)


def trade(message, totals, chips, arrivals):
    z = lax.axis_index("chip")
    lanes = message.shape[-1]
    data = message
    blocks, seen = chips, 1
    for step in range(chips.bit_length() - 1):
        mine = (z >> step) & 1
        data = data.reshape(blocks // 2, 2, seen, lanes)
        keep = lax.dynamic_index_in_dim(data, mine, 1, keepdims=False)
        give = lax.dynamic_index_in_dim(data, 1 - mine, 1, keepdims=False)
        rows = chips // 2
        packed = jnp.concatenate([give.reshape(rows, lanes), totals], axis=0)
        got = lax.ppermute(packed, "chip", [(i, i ^ (1 << step)) for i in range(chips)])
        got, _ = lax.optimization_barrier((got, arrivals[step]))
        totals = totals + got[rows:]
        came = got[:rows].reshape(blocks // 2, seen, lanes)
        low = jnp.where(mine == 0, keep, came)
        high = jnp.where(mine == 0, came, keep)
        data = jnp.stack([low, high], axis=1)
        blocks //= 2
        seen *= 2
    totals = totals + lax.ppermute(totals, "core", [(0, 1), (1, 0)])
    return data.reshape(chips, lanes), totals


def layer(tokens, router_weight, expert_ids):
    chips = lax.axis_size("chip")
    reach = chips // 2
    local_rows, width = tokens.shape
    half = width // 2
    per_dev = EXPERTS // (2 * chips)
    per_chip = 2 * per_dev
    slots_chip = per_chip * CAP
    z = lax.axis_index("chip")
    core = lax.axis_index("core")
    onward = [(i, (i + 1) % chips) for i in range(chips)]
    backward = [(i, (i - 1) % chips) for i in range(chips)]

    def send(x, to):
        return lax.ppermute(x, "chip", to)

    def swap(x):
        return lax.ppermute(x, "core", [(0, 1), (1, 0)])

    def need(h, far):
        if h <= reach - 3:
            return local_rows
        rows = slots_chip * (far - h + 1)
        return min(local_rows, (rows + 7) // 8 * 8)

    ids_t = expert_ids.T
    zs = z.astype(jnp.int32).reshape(1)
    sds = jax.ShapeDtypeStruct
    flows = whole_call(
        functools.partial(order_body, chips, per_chip), zs,
        (expert_ids, ids_t, tokens), [sds((local_rows, half), tokens.dtype)] * 4,
    )
    fars = (reach, reach - 1, reach - 1, reach)
    ways = (onward, onward, backward, backward)
    own, hops = flows[:2], []
    for h in range(1, reach + 1):
        sent = []
        for x, far, way in zip(flows, fars, ways):
            if h <= far:
                x = send(x[: need(h, far)], way)
                sent.append(x)
            else:
                sent.append(None)
        flows = sent
        hops.append([x for x in flows if x is not None])
    (table,) = whole_call(
        functools.partial(route_body, chips, per_chip), zs,
        (expert_ids, ids_t, tokens, router_weight), [sds((32, EXPERTS), jnp.float32)],
    )
    rows = 3 * CAP
    message = table[:rows].reshape(rows, chips, per_chip).transpose(1, 2, 0)
    message = message.reshape(chips, per_chip * rows)
    message = jnp.pad(message, ((0, 0), (0, 128 - per_chip * rows)))
    got, totals = trade(
        message, table[rows : rows + 2], chips, [arrived[2] for arrived in hops[: reach - 1]]
    )
    token_total = jnp.float32(local_rows * 2 * chips)
    loss = EXPERTS * jnp.sum(totals[0] * totals[1]) / (token_total * token_total * TOP_K)

    blank = jnp.array([-1.0, -1.0, 0.0], jnp.float32)
    got = got[:, : per_chip * rows].reshape(chips, 2, per_dev, 3, CAP)
    got = jnp.where(core == 0, got, got[:, ::-1]).reshape(chips, per_chip, 3, CAP)
    got = got.transpose(0, 1, 3, 2)
    void = jnp.broadcast_to(blank, got.shape)
    got = jnp.concatenate(
        [jnp.where(core == 0, got, void), jnp.where(core == 0, void, got)], axis=2
    ).reshape(chips // 4, 4, per_chip, 2 * CAP, 3)
    moved = []
    for q in range(4):
        lead = (2 * CAP * q) % 8
        shape = lambda n: (chips // 4, per_chip, n, 3)
        moved.append(
            jnp.concatenate(
                [
                    jnp.broadcast_to(blank, shape(lead)),
                    got[:, q],
                    jnp.broadcast_to(blank, shape(WIN - lead - 2 * CAP)),
                ],
                axis=2,
            )
        )
    windows = jnp.stack(moved, axis=1).reshape(chips, per_chip * WIN, 3)
    windows = jnp.pad(windows, ((0, 0), (0, 0), (0, 5)))

    shape = sds((per_dev, 2 * chips * CAP, width), tokens.dtype)
    out, (keep, give) = place(None, windows, [z], own, None, shape, per_dev)
    old = ([z], keep, swap(give))
    live, sources = [], []
    for h, arrived in enumerate(hops, 1):
        up, down = (z - h) % chips, (z + h) % chips
        live += arrived
        sources += [up, down] if h < reach else [up]
        if h == reach - 1:
            continue
        out, (keep, give) = place(out, windows, sources, live, old, shape, per_dev)
        old = (sources, keep, swap(give))
        live, sources = [], []
    out, _ = place(out, windows, [], [], old, shape, per_dev)
    return out, loss.reshape(1)


def solution(mesh):
    finer = Mesh(mesh.devices.reshape(mesh.shape["groups"], -1, 2), ALL)
    in_specs = (P(ALL, None), P(), P(ALL, None))
    out_specs = (P(EXPERT, "groups", None), P("groups"))
    return jax.shard_map(layer, mesh=finer, in_specs=in_specs, out_specs=out_specs, check_vma=False)
```
